256 devices in a mesh: beam: 4 (over y, x), freq: 32 (over z), sub: 2 (over core).
Axes of the slice: x: 2, y: 2, z: 32, core: 2. Of those that a mesh axis runs over, the one named last changes fastest.
The devices are a block of a 4x8x32 slice.
Arguments:
- spectrum: bfloat16 [64, 4194304], P('sub', ('beam', 'freq')), parts along dimension 1
- hit_mask: int32 [64, 32768], P('sub', ('beam', 'freq')), parts along dimension 1, may hold values from 0 to 1, as said below
- owner_map: int32 [4096], P(('beam', 'freq')), parts along dimension 0, may hold values from 0 to 1023, as said below
- median_bin: int32 [4096], P(('beam', 'freq')), parts along dimension 0, may hold values from 32 to 559
- mad_bin: int32 [4096], P(('beam', 'freq')), parts along dimension 0, may hold values from 4 to 15
Outputs:
- hit_snr: bfloat16 [32, 2, 16384, 128], P('freq', 'sub', 'beam'), parts along dimension 2
- hit_keys: int32 [32, 2, 16384], P('freq', 'sub', 'beam'), parts along dimension 2
- hit_excess: float32 [32, 2, 16384], P('freq', 'sub', 'beam'), parts along dimension 2
The draws below stay inside these ranges and needn't reach their ends.
There are 4 independent parts, one for each index of `beam`. The reference program is written for one: setup_inputs(seed, part) draws one part's arguments, and reference() takes and returns one part's arrays. A program takes and returns all parts, laid end to end along the dimension named above; each array names one. Nothing has to cross between parts.
Inputs may be any that keep to these rules, and one draw needn't show every extreme that they name: `hit_mask`: for each index of freq, each half of the drift rates and each owner, at most 128 hit blocks go from the first to the last; in every draw some owner gets exactly 128 from every index of freq and half. `owner_map`: A permutation of the slots 0 to 1023; the 32 coarse channels of one index of freq go 1 to each owner, and the slot of index f's coarse channel at each owner is f.
All inputs are finite; a program needn't handle non-finite values.
Results may differ from the reference program's by a relative error of at most 0.007.
Values may be sent and summed in bfloat16 or wider, within the bound.
No kernel may reach another device: no remote copies, remote signals or barrier semaphores. Data moves between devices by JAX's collectives and lax.ppermute only.
A program may use at most 64 MiB of HBM per device.

```python
import jax
import jax.numpy as jnp
from jax import lax

CHANNELS = 1048576
COARSE_WIDTH = 1024
BLOCK = 128
CAP = 128
DR_DEV = 32
DRIFTS = 64
COARSE = 1024
BPC = 8
NBLK = 8192
CD = 32
Q = 1
LIST = 4096
N_FREQ = 32
N_SUB = 2


def joint_draw(key):
    freq_count = COARSE // CD
    base = jax.random.fold_in(key, 101)
    parts = jax.random.split(base, 7)
    source_keys = jax.random.split(parts[0], freq_count)
    shuffled = jax.vmap(lambda one: jax.random.permutation(one, CD))(source_keys).astype(jnp.int32)
    source = jnp.arange(freq_count, dtype=jnp.int32)[:, None]
    owner = shuffled % freq_count
    local = source * Q + shuffled // freq_count
    owner_map = (owner * CD + local).reshape(COARSE).astype(jnp.int32)
    true_bin = jax.random.randint(parts[1], (COARSE,), 32, 160, dtype=jnp.int32)
    mad = jax.random.randint(parts[2], (COARSE,), 4, 16, dtype=jnp.int32)
    stale = (jax.random.randint(parts[3], (COARSE,), 0, 16, dtype=jnp.int32) == 0).astype(jnp.int32)
    median = true_bin + 400 * stale
    hot = jax.random.randint(parts[6], (), 0, freq_count, dtype=jnp.int32)
    dest = owner.reshape(COARSE)
    level = jax.random.randint(parts[4], (COARSE,), 0, 5, dtype=jnp.int32)
    limit = jnp.where(dest == hot, 1024, 32 * jnp.power(2, level)).astype(jnp.int32)
    tickets = jax.random.randint(parts[5], (DRIFTS, COARSE, BPC), 0, 1024, dtype=jnp.int32)
    raw = (tickets < limit[None, :, None]).astype(jnp.int32)
    half = (jnp.arange(DRIFTS, dtype=jnp.int32) // DR_DEV)[:, None, None]
    sender = (jnp.arange(COARSE, dtype=jnp.int32) // CD)[None, :, None]
    group = (half * freq_count + sender) * freq_count + dest[None, :, None]
    group = jnp.broadcast_to(group, (DRIFTS, COARSE, BPC)).reshape(-1)
    flat = raw.reshape(-1)
    groups_total = DRIFTS // DR_DEV * freq_count * freq_count
    order = jnp.argsort(group, stable=True)
    ordered = flat[order]
    running = jnp.cumsum(ordered).astype(jnp.int32)
    counts = jax.ops.segment_sum(flat, group, num_segments=groups_total)
    starts = (jnp.cumsum(counts) - counts).astype(jnp.int32)
    rank = running - starts[group[order]]
    keep = ordered * (rank <= CAP).astype(jnp.int32)
    mask = jnp.zeros_like(flat).at[order].set(keep).reshape(DRIFTS, COARSE, BPC)
    return (owner_map, median, mad, mask, true_bin)


def draw_owner_map(key, part):
    return joint_draw(key)[0]


def draw_median_bin(key, part):
    return joint_draw(key)[1]


def draw_mad_bin(key, part):
    return joint_draw(key)[2]


def draw_hit_mask(key, part):
    return joint_draw(key)[3].reshape(DRIFTS, NBLK)


def draw_spectrum(key, part):
    owner_map, median, mad, mask, true_bin = joint_draw(key)
    noise_key = jax.random.fold_in(key, 202)
    tone_key = jax.random.fold_in(key, 303)
    deviation = 1.4826 * 0.0625 * mad.astype(jnp.float32)
    center = 0.0625 * true_bin.astype(jnp.float32)
    ramp = 0.6 * jnp.power(3.0, jnp.arange(DRIFTS, dtype=jnp.float32) / max(DRIFTS - 1, 1))
    noise = jax.random.normal(noise_key, (DRIFTS, COARSE, BPC, BLOCK), jnp.float32)
    tone_at = jax.random.randint(tone_key, (DRIFTS, COARSE, BPC), 0, BLOCK, dtype=jnp.int32)
    tone = (jnp.arange(BLOCK, dtype=jnp.int32)[None, None, None, :] == tone_at[..., None]).astype(jnp.float32)
    tone = tone * mask[..., None].astype(jnp.float32)
    scale = deviation[None, :, None, None] * ramp[:, None, None, None]
    power = center[None, :, None, None] + scale * noise + 8.0 * scale * tone
    return power.reshape(DRIFTS, CHANNELS).astype(jnp.bfloat16)


def setup_inputs(seed: int = 0, part: int = 0) -> dict:
    key_of = jax.random.split(jax.random.key(seed), 6)
    own_keys = jax.random.split(jax.random.fold_in(key_of[5], part), 6)
    return {
        "spectrum": draw_spectrum(jax.random.fold_in(jax.random.fold_in(key_of[5], part), 71), part),
        "hit_mask": draw_hit_mask(jax.random.fold_in(jax.random.fold_in(key_of[5], part), 71), part),
        "owner_map": draw_owner_map(jax.random.fold_in(jax.random.fold_in(key_of[5], part), 71), part),
        "median_bin": draw_median_bin(jax.random.fold_in(jax.random.fold_in(key_of[5], part), 71), part),
        "mad_bin": draw_mad_bin(jax.random.fold_in(jax.random.fold_in(key_of[5], part), 71), part),
    }


BIN_STEP = 0.0625
MAD_WIDTH = 5.0
MAD_SCALE = 1.4826
THRESH = 3.0

def reference(spectrum, hit_mask, owner_map, median_bin, mad_bin):
    per_coarse = COARSE_WIDTH // BLOCK
    power = spectrum.astype(jnp.float32).reshape(DRIFTS, COARSE, COARSE_WIDTH)
    center = BIN_STEP * median_bin.astype(jnp.float32)
    spread = MAD_WIDTH * BIN_STEP * mad_bin.astype(jnp.float32)
    inside = (power >= (center - spread)[None, :, None]) & (power <= (center + spread)[None, :, None])
    kept = jnp.where(inside, power - center[None, :, None], jnp.float32(0.0))
    count = lax.optimization_barrier(jnp.sum(inside.astype(jnp.float32), axis=(0, 2)))
    first = lax.optimization_barrier(jnp.sum(kept, axis=(0, 2)))
    second = lax.optimization_barrier(jnp.sum(kept * kept, axis=(0, 2)))
    floor_count = jnp.maximum(count, 1.0)
    mean_level = center + first / floor_count
    mad_sigma = MAD_SCALE * BIN_STEP * mad_bin.astype(jnp.float32)
    sigma = jnp.sqrt(0.5 * second / floor_count + 0.5 * mad_sigma * mad_sigma)
    snr = ((power - mean_level[None, :, None]) / sigma[None, :, None]).astype(jnp.bfloat16)
    snr = snr.reshape(DRIFTS, COARSE, per_coarse, BLOCK)
    inverse = jnp.zeros((COARSE,), jnp.int32).at[owner_map].set(jnp.arange(COARSE, dtype=jnp.int32))
    by_slot = snr[:, inverse]
    marks = hit_mask.reshape(DRIFTS, COARSE, per_coarse)[:, inverse]
    by_slot = by_slot.reshape(N_SUB, DR_DEV, N_FREQ, CD, per_coarse, BLOCK).transpose(2, 0, 3, 1, 4, 5)
    by_slot = by_slot.reshape(N_FREQ * N_SUB, CD * DR_DEV * per_coarse, BLOCK)
    marks = marks.reshape(N_SUB, DR_DEV, N_FREQ, CD, per_coarse).transpose(2, 0, 3, 1, 4)
    marks = marks.reshape(N_FREQ * N_SUB, CD * DR_DEV * per_coarse).astype(jnp.int32)
    slots = jnp.arange(CD, dtype=jnp.int32)[None, None, :, None, None]
    halves = jnp.arange(N_SUB, dtype=jnp.int32)[None, :, None, None, None]
    drifts = jnp.arange(DR_DEV, dtype=jnp.int32)[None, None, None, :, None]
    blocks = jnp.arange(per_coarse, dtype=jnp.int32)[None, None, None, None, :]
    keys = (slots * DRIFTS + halves * DR_DEV + drifts) * per_coarse + blocks
    keys = jnp.broadcast_to(keys, (N_FREQ, N_SUB, CD, DR_DEV, per_coarse)).reshape(N_FREQ * N_SUB, -1)
    place = jnp.where(marks > 0, jnp.cumsum(marks, axis=-1).astype(jnp.int32) - 1, LIST).astype(jnp.int32)

    def collect(items):
        rows, key_row, place_row = items
        snr_list = jnp.zeros((LIST, BLOCK), jnp.bfloat16).at[place_row].set(rows, mode='drop')
        key_list = jnp.full((LIST,), -1, jnp.int32).at[place_row].set(key_row, mode='drop')
        excess = lax.optimization_barrier(jnp.sum(jnp.maximum(snr_list.astype(jnp.float32) - THRESH, 0.0), axis=-1))
        return (snr_list, key_list, excess)
    snr_lists, key_lists, excess = lax.map(collect, (by_slot, keys, place))
    return (snr_lists.reshape(N_FREQ, N_SUB, LIST, BLOCK), key_lists.reshape(N_FREQ, N_SUB, LIST), excess.reshape(N_FREQ, N_SUB, LIST))
```

```python
import functools

import jax
import jax.numpy as jnp
from jax import lax
from jax.experimental import pallas as pl
from jax.experimental.pallas import tpu as pltpu
from jax.sharding import PartitionSpec as P

COARSE_WIDTH = 1024
BLOCK = 128
CAP = 128
PER_COARSE = COARSE_WIDTH // BLOCK

BIN_STEP = 0.0625
MAD_WIDTH = 5.0
MAD_SCALE = 1.4826
THRESH = 3.0
LIMIT = 16 * 1024 * 1024

F32 = jnp.float32
BF16 = jnp.bfloat16


def iota(shape, axis):
    return lax.broadcasted_iota(jnp.int32, shape, axis)


def dot(a, b, dims=((1,), (0,))):
    return lax.dot_general(a, b, (dims, ((), ())), preferred_element_type=F32)


def pack_kernel(drifts, coarse, group, map_ref, mask_ref, spec_ref, out_ref, key_ref, rank_ref):
    step = pl.program_id(0)
    width = PER_COARSE * drifts

    @pl.when(step == 0)
    def _():
        marks = mask_ref[...].astype(F32).astype(BF16)
        row = jnp.zeros((coarse, width), F32)
        for b in range(PER_COARSE):
            pick = iota((coarse * PER_COARSE, coarse), 0) == iota(
                (coarse * PER_COARSE, coarse), 1
            ) * PER_COARSE + b
            of_block = dot(marks, jnp.where(pick, 1.0, 0.0).astype(BF16))
            place = iota((drifts, width), 1) == iota((drifts, width), 0) + b * drifts
            row += dot(
                of_block.astype(BF16), jnp.where(place, 1.0, 0.0).astype(BF16), ((0,), (0,))
            )
        order = lambda k: (k % drifts) * PER_COARSE + k // drifts
        before = order(iota((width, width), 0)) < order(iota((width, width), 1))
        rank = dot(row.astype(BF16), jnp.where(before, 1.0, 0.0).astype(BF16))
        rank_ref[...] = jnp.where(row > 0.5, rank, -1.0)

    slots = iota((CAP, width), 0).astype(F32)
    position = iota((width, CAP), 0)
    label = ((position % drifts) * PER_COARSE + position // drifts + 1).astype(F32).astype(BF16)
    diagonal = iota((CAP, CAP), 0) == iota((CAP, CAP), 1)
    for j in range(group):
        at = step * group + j
        owner = lax.div(map_ref[at], coarse)
        chosen = jnp.where(rank_ref[pl.ds(at, 1), :] == slots, 1.0, 0.0).astype(BF16)
        base = j * COARSE_WIDTH
        rows = jnp.concatenate(
            [spec_ref[:, base + b * BLOCK : base + (b + 1) * BLOCK] for b in range(PER_COARSE)],
            axis=0,
        )
        taken = dot(chosen, jnp.concatenate([rows, label], axis=1))
        out_ref[owner] = taken[:, :BLOCK].astype(BF16)
        key_ref[pl.ds(owner, 1), :] = jnp.sum(
            jnp.where(diagonal, taken[:, BLOCK:], 0.0), axis=0, keepdims=True
        )


def pack(spectrum, hit_mask, owner_map):
    drifts, channels = spectrum.shape
    coarse = owner_map.shape[0]
    group = 8
    return pl.pallas_call(
        functools.partial(pack_kernel, drifts, coarse, group),
        out_shape=(
            jax.ShapeDtypeStruct((coarse, CAP, BLOCK), BF16),
            jax.ShapeDtypeStruct((coarse, CAP), F32),
        ),
        grid_spec=pltpu.PrefetchScalarGridSpec(
            num_scalar_prefetch=1,
            grid=(coarse // group,),
            in_specs=[
                pl.BlockSpec((drifts, coarse * PER_COARSE), lambda i, m: (0, 0)),
                pl.BlockSpec((drifts, group * COARSE_WIDTH), lambda i, m: (0, i)),
            ],
            out_specs=[
                pl.BlockSpec((coarse, CAP, BLOCK), lambda i, m: (0, 0, 0)),
                pl.BlockSpec((coarse, CAP), lambda i, m: (0, 0)),
            ],
            scratch_shapes=[pltpu.VMEM((coarse, PER_COARSE * drifts), F32)],
        ),
        compiler_params=pltpu.CompilerParams(vmem_limit_bytes=LIMIT),
        name="pack",
    )(owner_map, hit_mask, spectrum)


def unpack_kernel(senders, steps, at_ref, meta_ref, rows_ref, snr_ref, key_ref, excess_ref, list_ref, keys_ref):
    step = pl.program_id(0)
    total = at_ref[senders]

    @pl.when(step == 0)
    def _():
        lane = iota((1, CAP), 1)
        half = at_ref[senders + 1]
        for f in range(senders):
            start = at_ref[f]
            stats = meta_ref[f, 1:2, :]
            raw = rows_ref[f].astype(F32)
            list_ref[pl.ds(start, CAP), :] = (raw - stats[:, 0:1]) * stats[:, 1:2]
            key = meta_ref[f, 0:1, :].astype(jnp.int32) + (f * 512 + half * 256 - 1)
            row = lax.div(start, CAP)
            shift = lax.rem(start, CAP)
            moved = pltpu.roll(key, shift, 1)
            keys_ref[pl.ds(row, 1), :] = jnp.where(
                lane >= shift, moved, keys_ref[pl.ds(row, 1), :]
            )
            keys_ref[pl.ds(row + 1, 1), :] = moved

    per = senders // steps
    ones = jnp.ones((2 * BLOCK, BLOCK), BF16)
    diagonal = iota((CAP, CAP), 0) == iota((CAP, CAP), 1)
    for j in range(per):
        row = step * per + j
        first = row * CAP
        block = list_ref[pl.ds(pl.multiple_of(first, CAP), CAP), :]
        live = iota((CAP, BLOCK), 0) + first < total
        value = jnp.where(live, block, 0.0).astype(BF16)
        snr_ref[0, 0, j * CAP : (j + 1) * CAP, :] = value
        over = jnp.maximum(value.astype(F32) - THRESH, 0.0)
        high = over.astype(BF16)
        low = (over - high.astype(F32)).astype(BF16)
        sums = dot(jnp.concatenate([high, low], axis=1), ones)
        excess_ref[pl.ds(row, 1), :] = jnp.sum(
            jnp.where(diagonal, sums, 0.0), axis=0, keepdims=True
        )
        key_ref[pl.ds(row, 1), :] = jnp.where(
            iota((1, CAP), 1) + first < total, keys_ref[pl.ds(row, 1), :], -1
        )


def unpack(at, meta, arrived):
    senders = arrived.shape[0]
    steps = 4
    total = senders * CAP
    return pl.pallas_call(
        functools.partial(unpack_kernel, senders, steps),
        out_shape=(
            jax.ShapeDtypeStruct((1, 1, total, BLOCK), BF16),
            jax.ShapeDtypeStruct((senders, CAP), jnp.int32),
            jax.ShapeDtypeStruct((senders, CAP), F32),
        ),
        grid_spec=pltpu.PrefetchScalarGridSpec(
            num_scalar_prefetch=1,
            grid=(steps,),
            in_specs=[
                pl.BlockSpec((senders, 2, CAP), lambda i, m: (0, 0, 0)),
                pl.BlockSpec((senders, CAP, BLOCK), lambda i, m: (0, 0, 0)),
            ],
            out_specs=[
                pl.BlockSpec((1, 1, total // steps, BLOCK), lambda i, m: (0, 0, i, 0)),
                pl.BlockSpec((senders, CAP), lambda i, m: (0, 0)),
                pl.BlockSpec((senders, CAP), lambda i, m: (0, 0)),
            ],
            scratch_shapes=[
                pltpu.VMEM((total, BLOCK), F32),
                pltpu.VMEM((senders + 8, CAP), jnp.int32),
            ],
        ),
        compiler_params=pltpu.CompilerParams(vmem_limit_bytes=LIMIT),
        name="unpack",
    )(at, meta, arrived)


def statistics(spectrum, median_bin, mad_bin):
    drifts = spectrum.shape[0]
    coarse = median_bin.shape[0]
    power = spectrum.astype(F32).reshape(drifts, coarse, COARSE_WIDTH)
    center = BIN_STEP * median_bin.astype(F32)
    spread = MAD_WIDTH * BIN_STEP * mad_bin.astype(F32)
    inside = (power >= (center - spread)[None, :, None]) & (
        power <= (center + spread)[None, :, None]
    )
    kept = jnp.where(inside, power - center[None, :, None], 0.0)
    count = jnp.sum(inside.astype(F32), axis=(0, 2))
    first = jnp.sum(kept, axis=(0, 2))
    second = jnp.sum(kept * kept, axis=(0, 2))
    mine = jnp.stack([count, first, second])
    pairs = lax.axis_size("sub")
    total = mine
    for k in range(1, pairs):
        total = total + lax.ppermute(mine, "sub", [(i, (i + k) % pairs) for i in range(pairs)])
    count, first, second = total[0], total[1], total[2]
    floor_count = jnp.maximum(count, 1.0)
    mean_level = center + first / floor_count
    mad_sigma = MAD_SCALE * BIN_STEP * mad_bin.astype(F32)
    sigma = jnp.sqrt(0.5 * second / floor_count + 0.5 * mad_sigma * mad_sigma)
    return mean_level, 1.0 / sigma


def per_device(spectrum, hit_mask, owner_map, median_bin, mad_bin):
    coarse = owner_map.shape[0]
    senders = lax.axis_size("freq")
    payload, labels = pack(spectrum, hit_mask, owner_map)
    spectrum, payload = lax.optimization_barrier((spectrum, payload))
    with jax.named_scope("payload"):
        arrived = lax.all_to_all(payload, "freq", 0, 0, tiled=True)
    mean_level, inverse = statistics(spectrum, median_bin, mad_bin)
    owner = owner_map // coarse
    mine = owner[None, :] == jnp.arange(senders, dtype=jnp.int32)[:, None]
    level_to = jnp.sum(jnp.where(mine, mean_level[None, :], 0.0), axis=1)
    inverse_to = jnp.sum(jnp.where(mine, inverse[None, :], 0.0), axis=1)
    lane = jnp.arange(CAP, dtype=jnp.int32)[None, :]
    stats = jnp.where(lane == 0, level_to[:, None], inverse_to[:, None])
    with jax.named_scope("meta"):
        meta = lax.all_to_all(jnp.stack([labels, stats], axis=1), "freq", 0, 0, tiled=True)
    got = jnp.sum((meta[:, 0, :] > 0.5).astype(jnp.int32), axis=1)
    rank = jnp.arange(senders, dtype=jnp.int32)
    starts = jnp.sum(jnp.where(rank[None, :] < rank[:, None], got[None, :], 0), axis=1)
    at = jnp.concatenate(
        [starts, jnp.sum(got)[None], lax.axis_index("sub").astype(jnp.int32)[None]]
    )
    snr, keys, excess = unpack(at, meta, arrived)
    total = senders * CAP
    return snr, keys.reshape(1, 1, total), excess.reshape(1, 1, total)


def solution(mesh):
    placed = (
        P("sub", ("beam", "freq")),
        P("sub", ("beam", "freq")),
        P(("beam", "freq")),
        P(("beam", "freq")),
        P(("beam", "freq")),
    )
    return jax.shard_map(
        per_device,
        mesh=mesh,
        in_specs=placed,
        out_specs=(
            P("freq", "sub", "beam", None),
            P("freq", "sub", "beam"),
            P("freq", "sub", "beam"),
        ),
        check_vma=False,
    )
```

```python
import functools

import jax
import jax.numpy as jnp
from jax import lax
from jax.experimental import pallas as pl
from jax.experimental.pallas import tpu as pltpu
from jax.sharding import PartitionSpec as P

COARSE_WIDTH = 1024
BLOCK = 128
CAP = 128
PER_COARSE = COARSE_WIDTH // BLOCK
EXTRA = 8
ROWS = CAP + EXTRA

BIN_STEP = 0.0625
MAD_WIDTH = 5.0
MAD_SCALE = 1.4826
THRESH = 3.0
LIMIT = 16 * 1024 * 1024

F32 = jnp.float32
BF16 = jnp.bfloat16


def iota(shape, axis):
    return lax.broadcasted_iota(jnp.int32, shape, axis)


def dot(a, b, dims=((1,), (0,))):
    return lax.dot_general(a, b, (dims, ((), ())), preferred_element_type=F32)


def split(value):
    high = value.astype(BF16).astype(F32)
    rest = value - high
    middle = rest.astype(BF16).astype(F32)
    return high, middle, rest - middle


def hit_ranks(marks, drifts, coarse):
    width = PER_COARSE * drifts
    row = jnp.zeros((coarse, width), F32)
    for b in range(PER_COARSE):
        pick = iota((coarse * PER_COARSE, coarse), 0) == iota(
            (coarse * PER_COARSE, coarse), 1
        ) * PER_COARSE + b
        of_block = dot(marks, jnp.where(pick, 1.0, 0.0).astype(BF16))
        place = iota((drifts, width), 1) == iota((drifts, width), 0) + b * drifts
        row += dot(of_block.astype(BF16), jnp.where(place, 1.0, 0.0).astype(BF16), ((0,), (0,)))
    order = lambda k: (k % drifts) * PER_COARSE + k // drifts
    before = order(iota((width, width), 0)) < order(iota((width, width), 1))
    rank = dot(row.astype(BF16), jnp.where(before, 1.0, 0.0).astype(BF16))
    return jnp.where(row > 0.5, rank, -1.0)


def pack_kernel(
    drifts, coarse, group,
    map_ref, median_ref, mad_ref, mask_hbm, spec_hbm, out_hbm,
    mask_ref, spec_ref, out_ref, rank_ref, key_ref, part_ref, extra_ref,
    mask_sem, spec_sem, out_sem, extra_sem,
):
    width = PER_COARSE * drifts
    span = group * COARSE_WIDTH
    fetch_mask = pltpu.make_async_copy(mask_hbm, mask_ref, mask_sem)
    fetch_mask.start()
    fetches = [
        pltpu.make_async_copy(
            spec_hbm.at[:, pl.ds(g * span, span)], spec_ref.at[:, pl.ds(g * span, span)], spec_sem.at[g]
        )
        for g in range(coarse // group)
    ]
    for fetch in fetches:
        fetch.start()
    fetch_mask.wait()
    rank_ref[...] = hit_ranks(mask_ref[...].astype(F32).astype(BF16), drifts, coarse)

    slots = iota((CAP, width), 0).astype(F32)
    position = iota((width, CAP), 0)
    label = ((position % drifts) * PER_COARSE + position // drifts + 1).astype(F32).astype(BF16)
    diagonal = iota((CAP, CAP), 0) == iota((CAP, CAP), 1)
    sends = []
    for at in range(coarse):
        if at % group == 0:
            fetches[at // group].wait()
        owner = lax.div(map_ref[at], coarse)
        chosen = jnp.where(rank_ref[at : at + 1, :] == slots, 1.0, 0.0).astype(BF16)
        base = at * COARSE_WIDTH
        blocks = [
            spec_ref[:, base + b * BLOCK : base + (b + 1) * BLOCK] for b in range(PER_COARSE)
        ]
        rows = jnp.concatenate(blocks, axis=0)
        taken = dot(chosen, jnp.concatenate([rows, label], axis=1))
        out_ref[at] = taken[:, :BLOCK].astype(BF16)
        send = pltpu.make_async_copy(
            out_ref.at[at], out_hbm.at[owner, pl.ds(0, CAP), :], out_sem.at[at]
        )
        send.start()
        sends.append(send)
        key_ref[pl.ds(owner, 1), :] = jnp.sum(
            jnp.where(diagonal, taken[:, BLOCK:], 0.0), axis=0, keepdims=True
        )
        center = BIN_STEP * median_ref[at].astype(F32)
        spread = MAD_WIDTH * BIN_STEP * mad_ref[at].astype(F32)
        low, high = center - spread, center + spread
        count = jnp.zeros((drifts, BLOCK), F32)
        first = jnp.zeros((drifts, BLOCK), F32)
        second = jnp.zeros((drifts, BLOCK), F32)
        for block in blocks:
            power = block.astype(F32)
            inside = (power >= low) & (power <= high)
            kept = jnp.where(inside, power - center, 0.0)
            count += jnp.where(inside, 1.0, 0.0)
            first += kept
            second += kept * kept
        for q, value in enumerate((count, first, second)):
            part_ref[q, pl.ds(owner, 1), :] = jnp.sum(value, axis=0, keepdims=True)
        fill = jnp.full((1, BLOCK), 1.0, F32)
        part_ref[3, pl.ds(owner, 1), :] = fill * center
        part_ref[4, pl.ds(owner, 1), :] = fill * mad_ref[at].astype(F32)

    lane = iota((coarse, BLOCK), 1)
    stats = jnp.zeros((coarse, BLOCK), F32)
    for q in range(3):
        for k, part in enumerate(split(jnp.sum(part_ref[q], axis=1, keepdims=True))):
            stats = jnp.where(lane == 3 * q + k, part, stats)
    for k, part in enumerate(split(part_ref[3])):
        stats = jnp.where(lane == 9 + k, part, stats)
    stats = jnp.where(lane == 12, part_ref[4], stats)
    line = iota((EXTRA, BLOCK), 0)
    for o in range(coarse):
        tile = jnp.where(
            line == 0, key_ref[o : o + 1, :], jnp.where(line == 1, stats[o : o + 1, :], 0.0)
        )
        extra_ref[o] = tile.astype(BF16)
    extra = pltpu.make_async_copy(extra_ref, out_hbm.at[:, pl.ds(CAP, EXTRA), :], extra_sem)
    extra.start()
    for send in sends:
        send.wait()
    extra.wait()


def pack(spectrum, hit_mask, owner_map, median_bin, mad_bin):
    drifts, channels = spectrum.shape
    coarse = owner_map.shape[0]
    group = 4
    smem = pl.BlockSpec(memory_space=pltpu.SMEM)
    hbm = pl.BlockSpec(memory_space=pl.ANY)
    return pl.pallas_call(
        functools.partial(pack_kernel, drifts, coarse, group),
        out_shape=jax.ShapeDtypeStruct((coarse, ROWS, BLOCK), BF16),
        in_specs=[smem, smem, smem, hbm, hbm],
        out_specs=hbm,
        scratch_shapes=[
            pltpu.VMEM((drifts, coarse * PER_COARSE), jnp.int32),
            pltpu.VMEM((drifts, channels), BF16),
            pltpu.VMEM((coarse, CAP, BLOCK), BF16),
            pltpu.VMEM((coarse, PER_COARSE * drifts), F32),
            pltpu.VMEM((coarse, CAP), F32),
            pltpu.VMEM((5, coarse, BLOCK), F32),
            pltpu.VMEM((coarse, EXTRA, BLOCK), BF16),
            pltpu.SemaphoreType.DMA,
            pltpu.SemaphoreType.DMA((coarse // group,)),
            pltpu.SemaphoreType.DMA((coarse,)),
            pltpu.SemaphoreType.DMA,
        ],
        name="pack",
    )(owner_map, median_bin, mad_bin, hit_mask, spectrum)


def unpack_kernel(
    senders, steps,
    at_ref, mine_ref, theirs_ref, rows_ref, snr_ref, key_ref, excess_ref, list_ref, keys_ref,
):
    step = pl.program_id(0)
    total = at_ref[senders]

    @pl.when(step == 0)
    def _():
        lane = iota((1, CAP), 1)
        half = at_ref[senders + 1]
        mine = mine_ref[...]
        both = mine + theirs_ref[...]
        floor_count = jnp.maximum(both[:, 0:1], 1.0)
        level = mine[:, 3:4] + both[:, 1:2] / floor_count
        mad_sigma = MAD_SCALE * BIN_STEP * mine[:, 4:5]
        sigma = jnp.sqrt(0.5 * both[:, 2:3] / floor_count + 0.5 * mad_sigma * mad_sigma)
        inverse = 1.0 / sigma
        for f in range(senders):
            start = at_ref[f]
            raw = rows_ref[f, :CAP, :].astype(F32)
            list_ref[pl.ds(start, CAP), :] = (raw - level[f : f + 1, :]) * inverse[f : f + 1, :]
            key = rows_ref[f, CAP : CAP + EXTRA, :].astype(F32)[0:1, :]
            key = key.astype(jnp.int32) + (f * 512 + half * 256 - 1)
            row = lax.div(start, CAP)
            shift = lax.rem(start, CAP)
            moved = pltpu.roll(key, shift, 1)
            keys_ref[pl.ds(row, 1), :] = jnp.where(
                lane >= shift, moved, keys_ref[pl.ds(row, 1), :]
            )
            keys_ref[pl.ds(row + 1, 1), :] = moved

    per = senders // steps
    ones = jnp.ones((2 * BLOCK, BLOCK), BF16)
    diagonal = iota((CAP, CAP), 0) == iota((CAP, CAP), 1)
    for j in range(per):
        row = step * per + j
        first = row * CAP
        block = list_ref[pl.ds(pl.multiple_of(first, CAP), CAP), :]
        live = iota((CAP, BLOCK), 0) + first < total
        value = jnp.where(live, block, 0.0).astype(BF16)
        snr_ref[0, 0, j * CAP : (j + 1) * CAP, :] = value
        over = jnp.maximum(value.astype(F32) - THRESH, 0.0)
        high = over.astype(BF16)
        low = (over - high.astype(F32)).astype(BF16)
        sums = dot(jnp.concatenate([high, low], axis=1), ones)
        excess_ref[pl.ds(row, 1), :] = jnp.sum(
            jnp.where(diagonal, sums, 0.0), axis=0, keepdims=True
        )
        key_ref[pl.ds(row, 1), :] = jnp.where(
            iota((1, CAP), 1) + first < total, keys_ref[pl.ds(row, 1), :], -1
        )


def unpack(at, mine, theirs, arrived):
    senders = arrived.shape[0]
    steps = 4
    total = senders * CAP
    return pl.pallas_call(
        functools.partial(unpack_kernel, senders, steps),
        out_shape=(
            jax.ShapeDtypeStruct((1, 1, total, BLOCK), BF16),
            jax.ShapeDtypeStruct((senders, CAP), jnp.int32),
            jax.ShapeDtypeStruct((senders, CAP), F32),
        ),
        grid_spec=pltpu.PrefetchScalarGridSpec(
            num_scalar_prefetch=1,
            grid=(steps,),
            in_specs=[
                pl.BlockSpec((senders, BLOCK), lambda i, m: (0, 0)),
                pl.BlockSpec((senders, BLOCK), lambda i, m: (0, 0)),
                pl.BlockSpec((senders, ROWS, BLOCK), lambda i, m: (0, 0, 0)),
            ],
            out_specs=[
                pl.BlockSpec((1, 1, total // steps, BLOCK), lambda i, m: (0, 0, i, 0)),
                pl.BlockSpec((senders, CAP), lambda i, m: (0, 0)),
                pl.BlockSpec((senders, CAP), lambda i, m: (0, 0)),
            ],
            scratch_shapes=[
                pltpu.VMEM((total, BLOCK), F32),
                pltpu.VMEM((senders + 8, CAP), jnp.int32),
            ],
        ),
        compiler_params=pltpu.CompilerParams(vmem_limit_bytes=LIMIT),
        name="unpack",
    )(at, mine, theirs, arrived)


def from_partner(value):
    pairs = lax.axis_size("sub")
    return lax.ppermute(value, "sub", [(i, (i + 1) % pairs) for i in range(pairs)])


def per_device(spectrum, hit_mask, owner_map, median_bin, mad_bin):
    senders = lax.axis_size("freq")
    payload = pack(spectrum, hit_mask, owner_map, median_bin, mad_bin)
    arrived = lax.all_to_all(payload, "freq", 0, 0, tiled=True)
    parts = arrived[:, CAP + 1, :].astype(F32)
    sums = [parts[:, 3 * q] + parts[:, 3 * q + 1] + parts[:, 3 * q + 2] for q in range(4)]
    mine = jnp.stack([*sums, parts[:, 12]], axis=1)
    mine = jnp.pad(mine, ((0, 0), (0, BLOCK - mine.shape[1])))
    theirs = from_partner(mine)
    got = jnp.sum((arrived[:, CAP, :].astype(F32) > 0.5).astype(jnp.int32), axis=1)
    rank = jnp.arange(senders, dtype=jnp.int32)
    starts = jnp.sum(jnp.where(rank[None, :] < rank[:, None], got[None, :], 0), axis=1)
    half = lax.axis_index("sub").astype(jnp.int32)
    at = jnp.concatenate([starts, jnp.stack([jnp.sum(got), half])])
    snr, keys, excess = unpack(at, mine, theirs, arrived)
    total = senders * CAP
    return snr, keys.reshape(1, 1, total), excess.reshape(1, 1, total)


def solution(mesh):
    placed = (
        P("sub", ("beam", "freq")),
        P("sub", ("beam", "freq")),
        P(("beam", "freq")),
        P(("beam", "freq")),
        P(("beam", "freq")),
    )
    return jax.shard_map(
        per_device,
        mesh=mesh,
        in_specs=placed,
        out_specs=(
            P("freq", "sub", "beam", None),
            P("freq", "sub", "beam"),
            P("freq", "sub", "beam"),
        ),
        check_vma=False,
    )
```

```python
import functools

import jax
import jax.numpy as jnp
from jax import lax
from jax.experimental import pallas as pl
from jax.experimental.pallas import tpu as pltpu
from jax.sharding import PartitionSpec as P

COARSE_WIDTH = 1024
BLOCK = 128
CAP = 128
PER_COARSE = COARSE_WIDTH // BLOCK
EXTRA = 2
ROWS = CAP + EXTRA

BIN_STEP = 0.0625
MAD_WIDTH = 5.0
MAD_SCALE = 1.4826
THRESH = 3.0
LIMIT = 16 * 1024 * 1024

F32 = jnp.float32
BF16 = jnp.bfloat16


def iota(shape, axis):
    return lax.broadcasted_iota(jnp.int32, shape, axis)


def dot(a, b, dims=((1,), (0,))):
    return lax.dot_general(a, b, (dims, ((), ())), preferred_element_type=F32)


def split(value):
    high = value.astype(BF16).astype(F32)
    rest = value - high
    middle = rest.astype(BF16).astype(F32)
    return high, middle, rest - middle


def hit_ranks(marks, drifts, coarse):
    width = PER_COARSE * drifts
    row = jnp.zeros((coarse, width), F32)
    for b in range(PER_COARSE):
        pick = iota((coarse * PER_COARSE, coarse), 0) == iota(
            (coarse * PER_COARSE, coarse), 1
        ) * PER_COARSE + b
        of_block = dot(marks, jnp.where(pick, 1.0, 0.0).astype(BF16))
        place = iota((drifts, width), 1) == iota((drifts, width), 0) + b * drifts
        row += dot(of_block.astype(BF16), jnp.where(place, 1.0, 0.0).astype(BF16), ((0,), (0,)))
    order = lambda k: (k % drifts) * PER_COARSE + k // drifts
    before = order(iota((width, width), 0)) < order(iota((width, width), 1))
    rank = dot(row.astype(BF16), jnp.where(before, 1.0, 0.0).astype(BF16))
    return jnp.where(row > 0.5, rank, -1.0)


def pack_kernel(
    drifts, coarse, group,
    map_ref, median_ref, mad_ref, mask_hbm, spec_hbm, out_hbm,
    mask_ref, spec_ref, out_ref, rank_ref, key_ref, part_ref, from_ref,
    mask_sem, spec_sem, out_sem,
):
    width = PER_COARSE * drifts
    fetch_mask = pltpu.make_async_copy(mask_hbm, mask_ref, mask_sem)
    fetch_mask.start()
    fetch = pltpu.make_async_copy(spec_hbm, spec_ref, spec_sem)
    fetch.start()
    for c in range(coarse):
        from_ref[lax.div(map_ref[c], coarse)] = c
    fetch_mask.wait()
    rank_ref[...] = hit_ranks(mask_ref[...].astype(F32).astype(BF16), drifts, coarse)

    slots = iota((CAP, width), 0).astype(F32)
    position = iota((width, CAP), 0)
    label = ((position % drifts) * PER_COARSE + position // drifts + 1).astype(F32).astype(BF16)
    diagonal = iota((CAP, CAP), 0) == iota((CAP, CAP), 1)
    lane = iota((group, BLOCK), 1)
    line = iota((EXTRA, BLOCK), 0)
    fetch.wait()
    sends = []
    for owner in range(coarse):
        c = from_ref[owner]
        chosen = jnp.where(rank_ref[pl.ds(c, 1), :] == slots, 1.0, 0.0).astype(BF16)
        blocks = [
            spec_ref[:, pl.ds(pl.multiple_of(c * COARSE_WIDTH + b * BLOCK, BLOCK), BLOCK)]
            for b in range(PER_COARSE)
        ]
        rows = jnp.concatenate(blocks, axis=0)
        taken = dot(chosen, jnp.concatenate([rows, label], axis=1))
        base = owner * ROWS
        out_ref[base : base + CAP, :] = taken[:, :BLOCK].astype(BF16)
        mine = owner % group
        key_ref[mine : mine + 1, :] = jnp.sum(
            jnp.where(diagonal, taken[:, BLOCK:], 0.0), axis=0, keepdims=True
        )
        mad = mad_ref[c].astype(F32)
        center = BIN_STEP * median_ref[c].astype(F32)
        spread = MAD_WIDTH * BIN_STEP * mad
        low, high = center - spread, center + spread
        count = jnp.zeros((drifts, BLOCK), F32)
        first = jnp.zeros((drifts, BLOCK), F32)
        second = jnp.zeros((drifts, BLOCK), F32)
        for block in blocks:
            power = block.astype(F32)
            inside = (power >= low) & (power <= high)
            kept = jnp.where(inside, power - center, 0.0)
            count += jnp.where(inside, 1.0, 0.0)
            first += kept
            second += kept * kept
        for q, value in enumerate((count, first, second)):
            part_ref[q, mine : mine + 1, :] = jnp.sum(value, axis=0, keepdims=True)
        part_ref[3, mine : mine + 1, :] = jnp.full((1, BLOCK), center, F32)
        part_ref[4, mine : mine + 1, :] = jnp.full((1, BLOCK), mad, F32)
        if mine + 1 < group:
            continue
        stats = jnp.where(lane == 12, part_ref[4], 0.0)
        for q in range(4):
            whole = jnp.sum(part_ref[q], axis=1, keepdims=True) if q < 3 else part_ref[q]
            for k, part in enumerate(split(whole)):
                stats = jnp.where(lane == 3 * q + k, part, stats)
        for k in range(group):
            tail = (owner - mine + k) * ROWS + CAP
            both = jnp.where(line == 0, key_ref[k : k + 1, :], stats[k : k + 1, :])
            out_ref[tail : tail + EXTRA, :] = both.astype(BF16)
        part = pl.ds((owner - mine) * ROWS, group * ROWS)
        send = pltpu.make_async_copy(
            out_ref.at[part, :], out_hbm.at[part, :], out_sem.at[owner // group]
        )
        send.start()
        sends.append(send)
    for send in sends:
        send.wait()


def pack(spectrum, hit_mask, owner_map, median_bin, mad_bin):
    drifts, channels = spectrum.shape
    coarse = owner_map.shape[0]
    group = 8
    smem = pl.BlockSpec(memory_space=pltpu.SMEM)
    hbm = pl.BlockSpec(memory_space=pl.ANY)
    return pl.pallas_call(
        functools.partial(pack_kernel, drifts, coarse, group),
        out_shape=jax.ShapeDtypeStruct((coarse * ROWS, BLOCK), BF16),
        in_specs=[smem, smem, smem, hbm, hbm],
        out_specs=hbm,
        scratch_shapes=[
            pltpu.VMEM((drifts, coarse * PER_COARSE), jnp.int32),
            pltpu.VMEM((drifts, channels), BF16),
            pltpu.VMEM((coarse * ROWS, BLOCK), BF16),
            pltpu.VMEM((coarse, PER_COARSE * drifts), F32),
            pltpu.VMEM((group, CAP), F32),
            pltpu.VMEM((5, group, BLOCK), F32),
            pltpu.SMEM((coarse,), jnp.int32),
            pltpu.SemaphoreType.DMA,
            pltpu.SemaphoreType.DMA,
            pltpu.SemaphoreType.DMA((coarse // group,)),
        ],
        name="pack",
    )(owner_map, median_bin, mad_bin, hit_mask, spectrum)


def unpack_kernel(
    senders, steps,
    half_ref, mine_ref, theirs_ref, rows_ref, snr_ref, key_ref, excess_ref,
    list_ref, keys_ref, label_ref, total_ref,
):
    step = pl.program_id(0)

    @pl.when(step == 0)
    def _():
        lane = iota((1, CAP), 1)
        half = half_ref[0]
        for f in range(senders):
            tail = f * ROWS + CAP
            label_ref[f : f + 1, :] = rows_ref[tail : tail + EXTRA, :].astype(F32)[0:1, :]
        label = label_ref[...]
        filled = jnp.sum(jnp.where(label > 0.5, 1.0, 0.0), axis=1, keepdims=True)
        before = iota((senders, senders), 1) < iota((senders, senders), 0)
        starts = dot(
            jnp.where(before, 1.0, 0.0).astype(BF16),
            jnp.broadcast_to(filled, (senders, BLOCK)).astype(BF16),
        ).astype(jnp.int32)
        total_ref[0] = starts[senders - 1, 0] + filled.astype(jnp.int32)[senders - 1, 0]
        mine = mine_ref[...]
        both = mine + theirs_ref[...]
        floor_count = jnp.maximum(both[:, 0:1], 1.0)
        level = mine[:, 3:4] + both[:, 1:2] / floor_count
        mad_sigma = MAD_SCALE * BIN_STEP * mine[:, 4:5]
        sigma = jnp.sqrt(0.5 * both[:, 2:3] / floor_count + 0.5 * mad_sigma * mad_sigma)
        inverse = 1.0 / sigma
        for f in range(senders):
            start = starts[f, 0]
            raw = rows_ref[f * ROWS : f * ROWS + CAP, :].astype(F32)
            list_ref[pl.ds(start, CAP), :] = (raw - level[f : f + 1, :]) * inverse[f : f + 1, :]
            key = label[f : f + 1, :].astype(jnp.int32) + (f * 512 + half * 256 - 1)
            row = lax.div(start, CAP)
            shift = lax.rem(start, CAP)
            moved = pltpu.roll(key, shift, 1)
            keys_ref[pl.ds(row, 1), :] = jnp.where(
                lane >= shift, moved, keys_ref[pl.ds(row, 1), :]
            )
            keys_ref[pl.ds(row + 1, 1), :] = moved

    total = total_ref[0]
    per = senders // steps
    ones = jnp.ones((2 * BLOCK, BLOCK), BF16)
    diagonal = iota((CAP, CAP), 0) == iota((CAP, CAP), 1)
    for j in range(per):
        row = step * per + j
        first = row * CAP
        block = list_ref[pl.ds(pl.multiple_of(first, CAP), CAP), :]
        live = iota((CAP, BLOCK), 0) + first < total
        value = jnp.where(live, block, 0.0).astype(BF16)
        snr_ref[0, 0, j * CAP : (j + 1) * CAP, :] = value
        over = jnp.maximum(value.astype(F32) - THRESH, 0.0)
        high = over.astype(BF16)
        low = (over - high.astype(F32)).astype(BF16)
        sums = dot(jnp.concatenate([high, low], axis=1), ones)
        excess_ref[pl.ds(row, 1), :] = jnp.sum(
            jnp.where(diagonal, sums, 0.0), axis=0, keepdims=True
        )
        key_ref[pl.ds(row, 1), :] = jnp.where(
            iota((1, CAP), 1) + first < total, keys_ref[pl.ds(row, 1), :], -1
        )


def unpack(half, mine, theirs, arrived):
    senders = mine.shape[0]
    steps = 4
    total = senders * CAP
    return pl.pallas_call(
        functools.partial(unpack_kernel, senders, steps),
        out_shape=(
            jax.ShapeDtypeStruct((1, 1, total, BLOCK), BF16),
            jax.ShapeDtypeStruct((senders, CAP), jnp.int32),
            jax.ShapeDtypeStruct((senders, CAP), F32),
        ),
        grid_spec=pltpu.PrefetchScalarGridSpec(
            num_scalar_prefetch=1,
            grid=(steps,),
            in_specs=[
                pl.BlockSpec((senders, BLOCK), lambda i, m: (0, 0)),
                pl.BlockSpec((senders, BLOCK), lambda i, m: (0, 0)),
                pl.BlockSpec((senders * ROWS, BLOCK), lambda i, m: (0, 0)),
            ],
            out_specs=[
                pl.BlockSpec((1, 1, total // steps, BLOCK), lambda i, m: (0, 0, i, 0)),
                pl.BlockSpec((senders, CAP), lambda i, m: (0, 0)),
                pl.BlockSpec((senders, CAP), lambda i, m: (0, 0)),
            ],
            scratch_shapes=[
                pltpu.VMEM((total, BLOCK), F32),
                pltpu.VMEM((senders + 8, CAP), jnp.int32),
                pltpu.VMEM((senders, CAP), F32),
                pltpu.SMEM((1,), jnp.int32),
            ],
        ),
        compiler_params=pltpu.CompilerParams(vmem_limit_bytes=LIMIT),
        name="unpack",
    )(half, mine, theirs, arrived)


def from_partner(value):
    pairs = lax.axis_size("sub")
    return lax.ppermute(value, "sub", [(i, (i + 1) % pairs) for i in range(pairs)])


def per_device(spectrum, hit_mask, owner_map, median_bin, mad_bin):
    senders = lax.axis_size("freq")
    payload = pack(spectrum, hit_mask, owner_map, median_bin, mad_bin)
    pairs = payload.reshape(senders, ROWS // 2, 2, BLOCK)
    arrived = lax.all_to_all(pairs, "freq", 0, 0, tiled=True)
    parts = arrived[:, CAP // 2, 1, :].astype(F32)
    sums = [parts[:, 3 * q] + parts[:, 3 * q + 1] + parts[:, 3 * q + 2] for q in range(4)]
    mine = jnp.stack([*sums, parts[:, 12]], axis=1)
    mine = jnp.pad(mine, ((0, 0), (0, BLOCK - mine.shape[1])))
    half = lax.axis_index("sub").astype(jnp.int32)
    snr, keys, excess = unpack(
        half[None], mine, from_partner(mine), arrived.reshape(payload.shape)
    )
    total = senders * CAP
    return snr, keys.reshape(1, 1, total), excess.reshape(1, 1, total)


def solution(mesh):
    placed = (
        P("sub", ("beam", "freq")),
        P("sub", ("beam", "freq")),
        P(("beam", "freq")),
        P(("beam", "freq")),
        P(("beam", "freq")),
    )
    return jax.shard_map(
        per_device,
        mesh=mesh,
        in_specs=placed,
        out_specs=(
            P("freq", "sub", "beam", None),
            P("freq", "sub", "beam"),
            P("freq", "sub", "beam"),
        ),
        check_vma=False,
    )
```

```python
import functools

import jax
import jax.numpy as jnp
from jax import lax
from jax.experimental import pallas as pl
from jax.experimental.pallas import tpu as pltpu
from jax.sharding import PartitionSpec as P

COARSE_WIDTH = 1024
BLOCK = 128
CAP = 128
PER_COARSE = COARSE_WIDTH // BLOCK
EXTRA = 2
ROWS = CAP + EXTRA

BIN_STEP = 0.0625
MAD_WIDTH = 5.0
MAD_SCALE = 1.4826
THRESH = 3.0
LIMIT = 16 * 1024 * 1024

F32 = jnp.float32
BF16 = jnp.bfloat16


def iota(shape, axis):
    return lax.broadcasted_iota(jnp.int32, shape, axis)


def dot(a, b, dims=((1,), (0,))):
    return lax.dot_general(a, b, (dims, ((), ())), preferred_element_type=F32)


def split(value):
    high = value.astype(BF16).astype(F32)
    rest = value - high
    middle = rest.astype(BF16).astype(F32)
    return high, middle, rest - middle


def hit_ranks(marks, drifts, coarse):
    width = PER_COARSE * drifts
    row = jnp.zeros((coarse, width), F32)
    for b in range(PER_COARSE):
        pick = iota((coarse * PER_COARSE, coarse), 0) == iota(
            (coarse * PER_COARSE, coarse), 1
        ) * PER_COARSE + b
        of_block = dot(marks, jnp.where(pick, 1.0, 0.0).astype(BF16))
        place = iota((drifts, width), 1) == iota((drifts, width), 0) + b * drifts
        row += dot(of_block.astype(BF16), jnp.where(place, 1.0, 0.0).astype(BF16), ((0,), (0,)))
    order = lambda k: (k % drifts) * PER_COARSE + k // drifts
    before = order(iota((width, width), 0)) < order(iota((width, width), 1))
    rank = dot(row.astype(BF16), jnp.where(before, 1.0, 0.0).astype(BF16))
    return jnp.where(row > 0.5, rank, -1.0)


def pack_kernel(
    drifts, coarse, group,
    map_hbm, median_hbm, mad_hbm, mask_hbm, spec_hbm, out_hbm,
    mask_ref, spec_ref, out_ref, rank_ref, key_ref, part_ref, from_ref, map_ref, median_ref, mad_ref,
    mask_sem, spec_sem, out_sem, small_sem,
):
    width = PER_COARSE * drifts
    small = [
        pltpu.make_async_copy(source, target, small_sem.at[i])
        for i, (source, target) in enumerate(
            [(map_hbm, map_ref), (median_hbm, median_ref), (mad_hbm, mad_ref)]
        )
    ]
    for copy in small:
        copy.start()
    fetch_mask = pltpu.make_async_copy(mask_hbm, mask_ref, mask_sem)
    fetch_mask.start()
    fetch = pltpu.make_async_copy(spec_hbm, spec_ref, spec_sem)
    fetch.start()
    for copy in small:
        copy.wait()
    for c in range(coarse):
        from_ref[lax.div(map_ref[c], coarse)] = c
    fetch_mask.wait()
    rank_ref[...] = hit_ranks(mask_ref[...].astype(F32).astype(BF16), drifts, coarse)

    slots = iota((CAP, width), 0).astype(F32)
    position = iota((width, CAP), 0)
    label = ((position % drifts) * PER_COARSE + position // drifts + 1).astype(F32).astype(BF16)
    diagonal = iota((CAP, CAP), 0) == iota((CAP, CAP), 1)
    lane = iota((group, BLOCK), 1)
    line = iota((EXTRA, BLOCK), 0)
    fetch.wait()
    sends = []
    for owner in range(coarse):
        c = from_ref[owner]
        chosen = jnp.where(rank_ref[pl.ds(c, 1), :] == slots, 1.0, 0.0).astype(BF16)
        blocks = [
            spec_ref[:, pl.ds(pl.multiple_of(c * COARSE_WIDTH + b * BLOCK, BLOCK), BLOCK)]
            for b in range(PER_COARSE)
        ]
        rows = jnp.concatenate(blocks, axis=0)
        taken = dot(chosen, jnp.concatenate([rows, label], axis=1))
        base = owner * ROWS
        out_ref[base : base + CAP, :] = taken[:, :BLOCK].astype(BF16)
        mine = owner % group
        key_ref[mine : mine + 1, :] = jnp.sum(
            jnp.where(diagonal, taken[:, BLOCK:], 0.0), axis=0, keepdims=True
        )
        mad = mad_ref[c].astype(F32)
        center = BIN_STEP * median_ref[c].astype(F32)
        spread = MAD_WIDTH * BIN_STEP * mad
        low, high = center - spread, center + spread
        count = jnp.zeros((drifts, BLOCK), F32)
        first = jnp.zeros((drifts, BLOCK), F32)
        second = jnp.zeros((drifts, BLOCK), F32)
        for block in blocks:
            power = block.astype(F32)
            inside = (power >= low) & (power <= high)
            kept = jnp.where(inside, power - center, 0.0)
            count += jnp.where(inside, 1.0, 0.0)
            first += kept
            second += kept * kept
        for q, value in enumerate((count, first, second)):
            part_ref[q, mine : mine + 1, :] = jnp.sum(value, axis=0, keepdims=True)
        part_ref[3, mine : mine + 1, :] = jnp.full((1, BLOCK), center, F32)
        part_ref[4, mine : mine + 1, :] = jnp.full((1, BLOCK), mad, F32)
        if mine + 1 < group:
            continue
        stats = jnp.where(lane == 12, part_ref[4], 0.0)
        for q in range(4):
            whole = jnp.sum(part_ref[q], axis=1, keepdims=True) if q < 3 else part_ref[q]
            for k, part in enumerate(split(whole)):
                stats = jnp.where(lane == 3 * q + k, part, stats)
        for k in range(group):
            tail = (owner - mine + k) * ROWS + CAP
            both = jnp.where(line == 0, key_ref[k : k + 1, :], stats[k : k + 1, :])
            out_ref[tail : tail + EXTRA, :] = both.astype(BF16)
        part = pl.ds((owner - mine) * ROWS, group * ROWS)
        send = pltpu.make_async_copy(
            out_ref.at[part, :], out_hbm.at[part, :], out_sem.at[owner // group]
        )
        send.start()
        sends.append(send)
    for send in sends:
        send.wait()


def pack(spectrum, hit_mask, owner_map, median_bin, mad_bin):
    drifts, channels = spectrum.shape
    coarse = owner_map.shape[0]
    group = 8
    smem = pl.BlockSpec(memory_space=pltpu.SMEM)
    hbm = pl.BlockSpec(memory_space=pl.ANY)
    return pl.pallas_call(
        functools.partial(pack_kernel, drifts, coarse, group),
        out_shape=jax.ShapeDtypeStruct((coarse * ROWS, BLOCK), BF16),
        in_specs=[hbm] * 5,
        out_specs=hbm,
        scratch_shapes=[
            pltpu.VMEM((drifts, coarse * PER_COARSE), jnp.int32),
            pltpu.VMEM((drifts, channels), BF16),
            pltpu.VMEM((coarse * ROWS, BLOCK), BF16),
            pltpu.VMEM((coarse, PER_COARSE * drifts), F32),
            pltpu.VMEM((group, CAP), F32),
            pltpu.VMEM((5, group, BLOCK), F32),
            pltpu.SMEM((coarse,), jnp.int32),
            pltpu.SMEM((coarse,), jnp.int32),
            pltpu.SMEM((coarse,), jnp.int32),
            pltpu.SMEM((coarse,), jnp.int32),
            pltpu.SemaphoreType.DMA,
            pltpu.SemaphoreType.DMA,
            pltpu.SemaphoreType.DMA((coarse // group,)),
            pltpu.SemaphoreType.DMA((3,)),
        ],
        name="pack",
    )(owner_map, median_bin, mad_bin, hit_mask, spectrum)


def unpack_kernel(
    senders, part,
    mine_ref, theirs_ref, rows_ref, snr_hbm, key_hbm, excess_hbm,
    list_ref, snr_ref, keys_ref, excess_ref, label_ref, snr_sem, key_sem, excess_sem,
):
    lane = iota((1, CAP), 1)
    half = lax.axis_index("sub")
    for f in range(senders):
        tail = f * ROWS + CAP
        label_ref[f : f + 1, :] = rows_ref[tail : tail + EXTRA, :].astype(F32)[0:1, :]
    label = label_ref[...]
    filled = jnp.sum(jnp.where(label > 0.5, 1.0, 0.0), axis=1, keepdims=True)
    before = iota((senders, senders), 1) < iota((senders, senders), 0)
    starts = dot(
        jnp.where(before, 1.0, 0.0).astype(BF16),
        jnp.broadcast_to(filled, (senders, BLOCK)).astype(BF16),
    ).astype(jnp.int32)
    total = starts[senders - 1, 0] + filled.astype(jnp.int32)[senders - 1, 0]
    mine, theirs = mine_ref[...].astype(F32), theirs_ref[...].astype(F32)
    whole = lambda v, q: sum(v[:, 3 * q + k : 3 * q + k + 1] for k in range(3))
    count, first, second = (whole(mine, q) + whole(theirs, q) for q in range(3))
    floor_count = jnp.maximum(count, 1.0)
    level = whole(mine, 3) + first / floor_count
    mad_sigma = MAD_SCALE * BIN_STEP * mine[:, 12:13]
    sigma = jnp.sqrt(0.5 * second / floor_count + 0.5 * mad_sigma * mad_sigma)
    inverse = 1.0 / sigma
    for f in range(senders):
        start = starts[f, 0]
        raw = rows_ref[f * ROWS : f * ROWS + CAP, :].astype(F32)
        list_ref[pl.ds(start, CAP), :] = (raw - level[f : f + 1, :]) * inverse[f : f + 1, :]
        key = label[f : f + 1, :].astype(jnp.int32) + (f * 512 + half * 256 - 1)
        row = lax.div(start, CAP)
        shift = lax.rem(start, CAP)
        moved = pltpu.roll(key, shift, 1)
        keys_ref[pl.ds(row, 1), :] = jnp.where(lane >= shift, moved, keys_ref[pl.ds(row, 1), :])
        keys_ref[pl.ds(row + 1, 1), :] = moved
    place = iota((senders, CAP), 0) * CAP + iota((senders, CAP), 1)
    keys_ref[:senders, :] = jnp.where(place < total, keys_ref[:senders, :], -1)
    copies = [pltpu.make_async_copy(keys_ref.at[pl.ds(0, senders), :], key_hbm, key_sem)]
    copies[0].start()

    ones = jnp.ones((2 * BLOCK, BLOCK), BF16)
    diagonal = iota((CAP, CAP), 0) == iota((CAP, CAP), 1)
    for row in range(senders):
        at = slice(row * CAP, (row + 1) * CAP)
        live = iota((CAP, BLOCK), 0) < total - row * CAP
        value = jnp.where(live, list_ref[at, :], 0.0).astype(BF16)
        snr_ref[at, :] = value
        if row % part == part - 1:
            done = pl.ds((row + 1 - part) * CAP, part * CAP)
            copies.append(
                pltpu.make_async_copy(
                    snr_ref.at[done, :], snr_hbm.at[0, 0, done, :], snr_sem.at[row // part]
                )
            )
            copies[-1].start()
        over = jnp.maximum(value.astype(F32) - THRESH, 0.0)
        high = over.astype(BF16)
        low = (over - high.astype(F32)).astype(BF16)
        sums = dot(jnp.concatenate([high, low], axis=1), ones)
        excess_ref[row : row + 1, :] = jnp.sum(
            jnp.where(diagonal, sums, 0.0), axis=0, keepdims=True
        )
    copies.append(pltpu.make_async_copy(excess_ref, excess_hbm, excess_sem))
    copies[-1].start()
    for copy in copies:
        copy.wait()


def unpack(mine, theirs, arrived):
    senders = mine.shape[0]
    part = 4
    total = senders * CAP
    vmem = pl.BlockSpec(memory_space=pltpu.VMEM)
    hbm = pl.BlockSpec(memory_space=pl.ANY)
    return pl.pallas_call(
        functools.partial(unpack_kernel, senders, part),
        out_shape=(
            jax.ShapeDtypeStruct((1, 1, total, BLOCK), BF16),
            jax.ShapeDtypeStruct((senders, CAP), jnp.int32),
            jax.ShapeDtypeStruct((senders, CAP), F32),
        ),
        in_specs=[vmem, vmem, vmem],
        out_specs=[hbm, hbm, hbm],
        scratch_shapes=[
            pltpu.VMEM((total, BLOCK), F32),
            pltpu.VMEM((total, BLOCK), BF16),
            pltpu.VMEM((senders + 8, CAP), jnp.int32),
            pltpu.VMEM((senders, CAP), F32),
            pltpu.VMEM((senders, CAP), F32),
            pltpu.SemaphoreType.DMA((senders // part,)),
            pltpu.SemaphoreType.DMA,
            pltpu.SemaphoreType.DMA,
        ],
        compiler_params=pltpu.CompilerParams(vmem_limit_bytes=LIMIT),
        name="unpack",
    )(mine, theirs, arrived)


def from_partner(value):
    pairs = lax.axis_size("sub")
    return lax.ppermute(value, "sub", [(i, (i + 1) % pairs) for i in range(pairs)])


def per_device(spectrum, hit_mask, owner_map, median_bin, mad_bin):
    senders = lax.axis_size("freq")
    payload = pack(spectrum, hit_mask, owner_map, median_bin, mad_bin)
    pairs = payload.reshape(senders, ROWS // 2, 2, BLOCK)
    arrived = lax.all_to_all(pairs, "freq", 0, 0, tiled=True)
    mine = arrived[:, CAP // 2, 1, :]
    snr, keys, excess = unpack(mine, from_partner(mine), arrived.reshape(payload.shape))
    total = senders * CAP
    return snr, keys.reshape(1, 1, total), excess.reshape(1, 1, total)


def solution(mesh):
    placed = (
        P("sub", ("beam", "freq")),
        P("sub", ("beam", "freq")),
        P(("beam", "freq")),
        P(("beam", "freq")),
        P(("beam", "freq")),
    )
    return jax.shard_map(
        per_device,
        mesh=mesh,
        in_specs=placed,
        out_specs=(
            P("freq", "sub", "beam", None),
            P("freq", "sub", "beam"),
            P("freq", "sub", "beam"),
        ),
        check_vma=False,
    )
```
